512 devices in a mesh: seq: 8 (over y_hi, x), col: 16 (over z), head: 4 (over y_lo, core).
Axes of the slice: x: 4, y: 4 (y_hi: 2, y_lo: 2; y = y_hi * 2 + y_lo), z: 16, core: 2. Of those that a mesh axis runs over, the one named last changes fastest.
Arguments:
- sequence_matrix: bfloat16 [128, 512, 256], P('seq', 'col'), may hold values from -24 to 24
- sequence_presence: int32 [128, 512], P('seq', 'col'), may hold values 0 or 1
- couple_matrix: bfloat16 [512, 512, 128], P('seq', 'col'), may hold values from -6 to 6
- couple_delta_selector: int32 [512, 512], P('seq', 'col'), may hold values 0 or 1
- softmax_scaling_vector: float32 [256], replicated, may hold values from 0.1 to 1.9
- couple_scaling_vector: float32 [128], replicated, may hold values from 0.1 to 1.9
- couple_logit_matrix: bfloat16 [128, 8], P(None, 'head'), may hold values from -44 to 44
- query_value_matrices: bfloat16 [256, 8, 128], P(None, 'head'), may hold values from -0.375 to 0.375
- merging_matrix: bfloat16 [256, 256], P('head'), may hold values from -0.375 to 0.375
- tensor_average_scaling: float32 [256], replicated, may hold values from 0.1 to 1.9
- factor_mapping_matrix: bfloat16 [256, 64], replicated, may hold values from -0.375 to 0.375
- tensor_average_matrix: bfloat16 [1024, 128], replicated, may hold values from -0.1875 to 0.1875
Outputs:
- sequence_refreshed: bfloat16 [128, 512, 256], P('seq', 'col')
- pair_output: bfloat16 [512, 512, 128], P('seq', 'col')
The draws below stay inside these ranges and needn't reach their ends.
All inputs are finite; a program needn't handle non-finite values. No bound on the sum of `sequence_presence` or of `couple_delta_selector` on one device may be relied on, other than what follows from the above.
Results may differ from the reference program's by a relative error of at most 0.005.
The reference program's roundings to bfloat16 on the way count: a program that leaves them out, or rounds other values in their place, can miss the bound.
Values may be sent and summed in bfloat16 or wider, within the bound.
No kernel may reach another device: no remote copies, remote signals or barrier semaphores. Data moves between devices by JAX's collectives and lax.ppermute only.
A program may use at most 64 MiB of HBM per device.

```python
import math
import jax
import jax.numpy as jnp
from jax import lax

FEATURE_WIDTH = 256
CZ = 128
ATTENDER_TOTAL = 8
ATTENDER_WIDTH = 32
FACTOR_WIDTH_SZ = 32
SEQUENCE_TOTAL = 128
POSITION_TOTAL = 512


def draw_sequence_matrix(key, part):
    sequence_summary = jax.random.normal(jax.random.fold_in(key, 11), (POSITION_TOTAL, FEATURE_WIDTH), jnp.float32)
    stability_epsilon = jax.random.normal(jax.random.fold_in(key, 12), (SEQUENCE_TOTAL, POSITION_TOTAL, FEATURE_WIDTH), jnp.float32)
    values_f = 0.8 * sequence_summary[None] + 0.6 * stability_epsilon
    return jnp.clip(values_f, -6.0, 6.0).astype(jnp.bfloat16)


def draw_couple_logit_matrix(key, part):
    entries = jnp.clip(jax.random.normal(jax.random.fold_in(key, 21), (CZ, ATTENDER_TOTAL), jnp.float32), -4.0, 4.0)
    lower_end = math.log(0.05)
    upper_end = math.log(0.25)
    scales = jnp.exp(jax.random.uniform(jax.random.fold_in(key, 22), (1, ATTENDER_TOTAL), jnp.float32, lower_end, upper_end))
    return (entries * scales).astype(jnp.bfloat16)


def touch_ends(drawn, key, least, top_value):
    longest = drawn.shape.index(max(drawn.shape))
    spots = []
    for shift in (0, 1):
        where = [jax.random.randint(jax.random.fold_in(key, axis), (), 0, length) for axis, length in enumerate(drawn.shape)]
        where[longest] = (where[longest] + shift) % drawn.shape[longest]
        spots.append(tuple(where))
    return drawn.at[spots[0]].set(least).at[spots[1]].set(top_value)


def block_scale(rng, dims, cuts, least, top_value):
    factor_of = 1.0
    for position, shards_of in cuts:
        steps = jax.random.uniform(jax.random.fold_in(jax.random.fold_in(rng, 6), position), (shards_of,), jnp.float32, least / len(cuts), top_value / len(cuts))
        factor_of = factor_of * jnp.repeat(jnp.exp(steps), dims[position] // shards_of).reshape((-1,) + (1,) * (len(dims) - 1 - position))
    return factor_of


def bell_draw(rng, dims, spread, limit, pieces=(), dtype=jnp.bfloat16):
    loudness = block_scale(rng, dims, pieces, -0.22, 0.18) if pieces else 1.0
    array = jax.random.normal(rng, dims, jnp.float32) * spread * loudness
    return jnp.minimum(jnp.maximum(array, -limit), limit).astype(dtype)


def setup_inputs(seed: int = 0) -> dict:
    streams_of = jax.random.split(jax.random.key(seed), 13)
    sequence_matrix = draw_sequence_matrix(jax.random.fold_in(streams_of[12], 71), 0)
    sequence_presence = touch_ends((jax.random.randint(streams_of[1], (SEQUENCE_TOTAL, POSITION_TOTAL), 0, 8) < 7).astype(jnp.int32), jax.random.fold_in(streams_of[1], 1), 0, 1)
    couple_matrix = bell_draw(streams_of[2], (POSITION_TOTAL, POSITION_TOTAL, CZ), 1.0, 6.0, ((0, 8), (1, 16)))
    couple_delta_selector = touch_ends((jax.random.randint(streams_of[3], (POSITION_TOTAL, POSITION_TOTAL), 0, 4) < 3).astype(jnp.int32), jax.random.fold_in(streams_of[3], 1), 0, 1)
    softmax_scaling_vector = jnp.clip(1.0 + 0.18 * jax.random.normal(streams_of[4], (FEATURE_WIDTH,), jnp.float32), 0.1, 1.9)
    couple_scaling_vector = jnp.clip(1.0 + 0.18 * jax.random.normal(streams_of[5], (CZ,), jnp.float32), 0.1, 1.9)
    couple_logit_matrix = draw_couple_logit_matrix(jax.random.fold_in(streams_of[12], 71), 0)
    query_value_matrices = bell_draw(streams_of[7], (FEATURE_WIDTH, ATTENDER_TOTAL, 4 * ATTENDER_WIDTH), FEATURE_WIDTH ** -0.5, 0.375, ((1, 4),))
    merging_matrix = bell_draw(streams_of[8], (ATTENDER_TOTAL * ATTENDER_WIDTH, FEATURE_WIDTH), (ATTENDER_TOTAL * ATTENDER_WIDTH) ** -0.5, 0.375, ((0, 4),))
    tensor_average_scaling = jnp.clip(1.0 + 0.18 * jax.random.normal(streams_of[9], (FEATURE_WIDTH,), jnp.float32), 0.1, 1.9)
    factor_mapping_matrix = bell_draw(streams_of[10], (FEATURE_WIDTH, 2 * FACTOR_WIDTH_SZ), FEATURE_WIDTH ** -0.5, 0.375)
    tensor_average_matrix = bell_draw(streams_of[11], (FACTOR_WIDTH_SZ * FACTOR_WIDTH_SZ, CZ), (FACTOR_WIDTH_SZ * FACTOR_WIDTH_SZ) ** -0.5, 0.1875)
    return dict(sequence_matrix=sequence_matrix, sequence_presence=sequence_presence, couple_matrix=couple_matrix, couple_delta_selector=couple_delta_selector, softmax_scaling_vector=softmax_scaling_vector, couple_scaling_vector=couple_scaling_vector, couple_logit_matrix=couple_logit_matrix, query_value_matrices=query_value_matrices, merging_matrix=merging_matrix, tensor_average_scaling=tensor_average_scaling, factor_mapping_matrix=factor_mapping_matrix, tensor_average_matrix=tensor_average_matrix)


EPSILON = 1e-05
MASKED_FILL = -1000000000.0

def standardize_features(input_arrays, gain_vec):
    values_f = input_arrays.astype(jnp.float32)
    average = lax.optimization_barrier(jnp.mean(values_f, axis=-1, keepdims=True))
    centered = values_f - average
    variance = lax.optimization_barrier(jnp.mean(centered * centered, axis=-1, keepdims=True))
    return centered * lax.rsqrt(variance + EPSILON) * gain_vec.astype(jnp.float32)

def reference(sequence_matrix, sequence_presence, couple_matrix, couple_delta_selector, softmax_scaling_vector, couple_scaling_vector, couple_logit_matrix, query_value_matrices, merging_matrix, tensor_average_scaling, factor_mapping_matrix, tensor_average_matrix):
    pair_normed = standardize_features(couple_matrix, couple_scaling_vector).astype(jnp.bfloat16)
    bias_flat = jnp.dot(pair_normed.reshape(POSITION_TOTAL * POSITION_TOTAL, CZ), couple_logit_matrix, preferred_element_type=jnp.float32)
    bias_rounded = lax.optimization_barrier(bias_flat.astype(jnp.bfloat16))
    bias_plane = bias_rounded.astype(jnp.float32).reshape(POSITION_TOTAL, POSITION_TOTAL, ATTENDER_TOTAL).transpose(2, 0, 1)
    absent_target_penalty = ((1 - sequence_presence).astype(jnp.float32) * MASKED_FILL).astype(jnp.bfloat16)
    score_scale = ATTENDER_WIDTH ** (-0.5)
    sequences_within_tile = 16
    linear_mapped = query_value_matrices.reshape(FEATURE_WIDTH, ATTENDER_TOTAL * 4 * ATTENDER_WIDTH)

    def sequence_softmax_step(input_arrays):
        alignment_block, block_mask = input_arrays
        standardized_source = standardize_features(alignment_block, softmax_scaling_vector).astype(jnp.bfloat16)
        linear_mapped_values = jnp.dot(standardized_source.reshape(sequences_within_tile * POSITION_TOTAL, FEATURE_WIDTH), linear_mapped, preferred_element_type=jnp.float32)
        linear_mapped_values = lax.optimization_barrier(linear_mapped_values.astype(jnp.bfloat16))
        linear_mapped_values = linear_mapped_values.astype(jnp.float32).reshape(sequences_within_tile, POSITION_TOTAL, ATTENDER_TOTAL, 4 * ATTENDER_WIDTH)
        query_part = linear_mapped_values[..., :ATTENDER_WIDTH]
        key_part = linear_mapped_values[..., ATTENDER_WIDTH:2 * ATTENDER_WIDTH]
        value_part = linear_mapped_values[..., 2 * ATTENDER_WIDTH:3 * ATTENDER_WIDTH]
        gate_part = linear_mapped_values[..., 3 * ATTENDER_WIDTH:]
        scores = jnp.einsum('sihd,sjhd->shij', query_part, key_part) * score_scale
        scores = scores + bias_plane[None] + block_mask.astype(jnp.float32)[:, None, None, :]
        weights = jax.nn.softmax(scores, axis=-1).astype(jnp.bfloat16)
        weights = lax.optimization_barrier(weights).astype(jnp.float32)
        attended = jnp.einsum('shij,sjhd->sihd', weights, value_part)
        gated = (jax.nn.sigmoid(gate_part) * attended).astype(jnp.bfloat16)
        return gated.reshape(sequences_within_tile, POSITION_TOTAL, ATTENDER_TOTAL * ATTENDER_WIDTH)
    tile_number = SEQUENCE_TOTAL // sequences_within_tile
    sigmoid_scaled_result = lax.map(sequence_softmax_step, (sequence_matrix.reshape(tile_number, sequences_within_tile, POSITION_TOTAL, FEATURE_WIDTH), absent_target_penalty.reshape(tile_number, sequences_within_tile, POSITION_TOTAL)))
    couple_delta = jnp.dot(sigmoid_scaled_result.reshape(SEQUENCE_TOTAL * POSITION_TOTAL, ATTENDER_TOTAL * ATTENDER_WIDTH), merging_matrix, preferred_element_type=jnp.float32)
    sequence_refreshed = (sequence_matrix.reshape(SEQUENCE_TOTAL * POSITION_TOTAL, FEATURE_WIDTH).astype(jnp.float32) + couple_delta).astype(jnp.bfloat16).reshape(SEQUENCE_TOTAL, POSITION_TOTAL, FEATURE_WIDTH)
    mask_as_float = sequence_presence.astype(jnp.float32)
    tensor_average_standardized = standardize_features(sequence_refreshed, tensor_average_scaling).astype(jnp.bfloat16)
    factor_vectors = jnp.dot(tensor_average_standardized.reshape(SEQUENCE_TOTAL * POSITION_TOTAL, FEATURE_WIDTH), factor_mapping_matrix, preferred_element_type=jnp.float32)
    factor_vectors = (factor_vectors.reshape(SEQUENCE_TOTAL, POSITION_TOTAL, 2 * FACTOR_WIDTH_SZ) * mask_as_float[..., None]).astype(jnp.bfloat16)
    factor_vectors = lax.optimization_barrier(factor_vectors).astype(jnp.float32)
    left_part = factor_vectors[..., :FACTOR_WIDTH_SZ]
    right_part = factor_vectors[..., FACTOR_WIDTH_SZ:]
    pair_count = jnp.dot(mask_as_float.T, mask_as_float, precision=lax.Precision.HIGHEST)
    block_res = POSITION_TOTAL // 8

    def project(left_block):
        outer_sum = jnp.einsum('sip,sjq->ijpq', left_block, right_part, precision=lax.Precision.HIGHEST)
        outer_sum = outer_sum.astype(jnp.bfloat16).reshape(block_res * POSITION_TOTAL, FACTOR_WIDTH_SZ * FACTOR_WIDTH_SZ)
        return jnp.dot(outer_sum, tensor_average_matrix, preferred_element_type=jnp.float32).reshape(block_res, POSITION_TOTAL, CZ)
    left_blocks = left_part.reshape(SEQUENCE_TOTAL, 8, block_res, FACTOR_WIDTH_SZ).transpose(1, 0, 2, 3)
    projected_pair = lax.map(project, left_blocks).reshape(POSITION_TOTAL, POSITION_TOTAL, CZ)
    pair_update = projected_pair / (1.0 + pair_count)[..., None] * couple_delta_selector.astype(jnp.float32)[..., None]
    pair_output = (couple_matrix.astype(jnp.float32) + pair_update).astype(jnp.bfloat16)
    return (sequence_refreshed, pair_output)
```

```python
import jax
import jax.numpy as jnp
from jax import lax
from jax.experimental import pallas as pl
from jax.experimental.pallas import tpu as pltpu
from jax.sharding import Mesh
from jax.sharding import PartitionSpec as P

SEQ = ("seq_0", "seq_1")
EPSILON = 1e-05
MASKED_FILL = -1000000000.0
F32 = jnp.float32
BF16 = jnp.bfloat16

SEQS, COLS, HEADS = 8, 16, 4
ROWS, POS, WIDTH = 16, 32, 256
TILE_I, TILE_J, PAIR = 64, 32, 128
ALL_POS = COLS * POS
OWN_POS = ALL_POS // HEADS
D = 32


def iota(shape, dim):
    return lax.broadcasted_iota(jnp.int32, shape, dim)


def dot(a, b):
    return jnp.dot(a, b, preferred_element_type=F32)


def dot_first(a, b):
    return lax.dot_general(a, b, (((0,), (0,)), ((), ())), preferred_element_type=F32)


def one_hot(mask):
    return mask.astype(F32).astype(BF16)


def normed(values, gain, width):
    average = jnp.sum(values, axis=-1, keepdims=True) * (1.0 / width)
    centered = values - average
    variance = jnp.sum(centered * centered, axis=-1, keepdims=True) * (1.0 / width)
    return centered * lax.rsqrt(variance + EPSILON) * gain


def vmem_call(kernel, out_shapes, *args, scalars=(), scratch=(), flops=1000000, name=None):
    specs = [pl.BlockSpec(memory_space=pltpu.SMEM)] * len(scalars)
    specs += [pl.BlockSpec(memory_space=pltpu.VMEM)] * len(args)
    single = not isinstance(out_shapes, (list, tuple))
    shapes = [out_shapes] if single else list(out_shapes)
    found = pl.pallas_call(
        kernel,
        out_shape=shapes,
        in_specs=specs,
        out_specs=[pl.BlockSpec(memory_space=pltpu.VMEM)] * len(shapes),
        scratch_shapes=list(scratch),
        cost_estimate=pl.CostEstimate(flops=flops, bytes_accessed=1000000, transcendentals=0),
        compiler_params=pltpu.CompilerParams(vmem_limit_bytes=48 * 1024 * 1024),
        name=name,
    )(*scalars, *args)
    return found[0] if single else found


def shape_of(dims, dtype=BF16):
    return jax.ShapeDtypeStruct(dims, dtype)


Z1_ROWS = 2 * POS + TILE_J + ROWS


def first_kernel(place, msa, presence, couple, gain, logits, out):
    col = place[0]
    low_lane = iota((PAIR, PAIR), 1) < TILE_I
    columns = logits[...].astype(F32)
    spread = jnp.where(low_lane, columns[:, 0:1], columns[:, 1:2]).astype(BF16)
    pair_gain = gain[...]
    step = 8
    place_of_lane = iota((TILE_J, PAIR), 1) % TILE_I

    def body(k, total):
        block = couple[pl.ds(k * step, step)].astype(F32).reshape(step * TILE_J, PAIR)
        value = normed(block, pair_gain, PAIR).astype(BF16)
        found = dot(value, spread)
        for r in range(step):
            row = found[r * TILE_J : (r + 1) * TILE_J]
            total = total + jnp.where(place_of_lane == k * step + r, row, 0.0)
        return total

    bias = lax.fori_loop(0, TILE_I // step, body, jnp.zeros((TILE_J, PAIR), F32))
    bias = bias.astype(BF16)
    marks = presence[...].astype(F32)
    marks = jnp.concatenate([marks] * 4, axis=1)
    marks = jnp.where(iota((ROWS, PAIR), 1) // POS == col % 4, marks, 0.0).astype(BF16)
    out[:, 0:POS, :] = msa[:, :, 0:128]
    out[:, POS : 2 * POS, :] = msa[:, :, 128:256]
    for dest in range(COLS):
        out[dest, 2 * POS : 2 * POS + TILE_J, :] = bias
        out[dest, 2 * POS + TILE_J :, :] = marks


def present_tile(first, t):
    at = 2 * POS + TILE_J
    total = first[4 * t, at:, :].astype(F32)
    for k in range(1, 4):
        total = total + first[4 * t + k, at:, :].astype(F32)
    return total.astype(BF16)


S1_ROWS = ALL_POS + 4 * ROWS


def spread_kernel(first, out):
    strip = first[:, 2 * POS : 2 * POS + TILE_J, :].reshape(ALL_POS, PAIR)
    tiles = [present_tile(first, t) for t in range(4)]
    for dest in range(SEQS):
        out[dest, 0:ALL_POS, :] = strip
        for t in range(4):
            out[dest, ALL_POS + ROWS * t : ALL_POS + ROWS * (t + 1), :] = tiles[t]


H1_ROWS = OWN_POS // 2 + 2 * 2 * D


def attend_kernel(place, first, strips, weights, gain, merging, keep, out, residual, marks, factor):
    seq, col, head = place[0], place[1], place[2]
    raw = jnp.concatenate(
        [
            first[:, 0:POS, :].reshape(ALL_POS, 128),
            first[:, POS : 2 * POS, :].reshape(ALL_POS, 128),
        ],
        axis=1,
    ).astype(F32)
    standard = normed(raw, gain[...], WIDTH).astype(BF16)
    both = jnp.concatenate([weights[0], weights[1]], axis=1)
    projected = dot(standard, both)
    rounded = projected.astype(BF16)
    turned = rounded.astype(F32).T

    own_row = one_hot(iota((ROWS, 128), 0) == col)
    row_marks = jnp.concatenate(
        [dot_first(present_tile(first, t), own_row) for t in range(4)], axis=0
    )
    key_bias = ((1.0 - row_marks) * MASKED_FILL).astype(BF16).astype(F32)

    by_owner = raw.reshape(COLS, HEADS, 8, WIDTH)
    marks_by_owner = row_marks.reshape(COLS, HEADS, 8, 128)
    own = jnp.zeros((COLS, 8, WIDTH), F32)
    own_marks = jnp.zeros((COLS, 8, 128), F32)
    for k in range(HEADS):
        own = own + jnp.where(head == k, by_owner[:, k], 0.0)
        own_marks = own_marks + jnp.where(head == k, marks_by_owner[:, k], 0.0)
    residual[...] = own.reshape(OWN_POS, WIDTH).astype(BF16)
    marks[...] = own_marks.reshape(OWN_POS, 128)

    rows_i = jnp.zeros((SEQS * ROWS, TILE_I), F32)
    rows_j = jnp.zeros((SEQS * ROWS, TILE_J), F32)
    for t in range(4):
        at = ALL_POS + ROWS * t
        tile = strips[:, at : at + ROWS, :].reshape(SEQS * ROWS, 128)
        lane = iota((128, TILE_I), 0) + 128 * t
        rows_i = rows_i + dot(tile, one_hot(lane == seq * TILE_I + iota((128, TILE_I), 1)))
        lane = iota((128, TILE_J), 0) + 128 * t
        rows_j = rows_j + dot(tile, one_hot(lane == col * TILE_J + iota((128, TILE_J), 1)))
    count = dot_first(rows_j.astype(BF16), rows_i.astype(BF16))
    same = one_hot(iota((TILE_I, TILE_I), 0) == iota((TILE_I, TILE_I), 1))
    kept = dot_first(keep[...].astype(F32).astype(BF16), same)
    factor[...] = kept / (1.0 + count)

    score_scale = D ** (-0.5)
    low = iota((D, 128), 1) < TILE_I
    zero = jnp.zeros((D, 128), F32)
    values = jnp.concatenate([turned[2 * D : 3 * D], turned[6 * D : 7 * D]], axis=0).astype(BF16)

    def tile_attended(a, first_queries, second_queries):
        queries = jnp.concatenate(
            [
                zero,
                jnp.where(low, first_queries, 0.0),
                zero,
                zero,
                zero,
                jnp.where(low, 0.0, second_queries),
                zero,
                zero,
            ],
            axis=0,
        ).astype(BF16)
        scores = dot(rounded, queries) * score_scale
        scores = scores + strips[a, 0:ALL_POS, :].astype(F32) + key_bias
        top = jnp.max(scores, axis=0, keepdims=True)
        raised = jnp.exp(scores - top)
        shares = (raised / jnp.sum(raised, axis=0, keepdims=True)).astype(BF16)
        return dot(values, shares)

    pieces = []
    for t in range(4):
        at = slice(128 * t, 128 * (t + 1))
        q0, q1 = turned[0:D, at], turned[4 * D : 5 * D, at]
        even = tile_attended(2 * t, q0, pltpu.roll(q1, 64, 1))
        odd = tile_attended(2 * t + 1, pltpu.roll(q0, 64, 1), q1)
        head_0 = jnp.where(low, even[0:D], pltpu.roll(odd[0:D], 64, 1))
        head_1 = jnp.where(low, pltpu.roll(even[D:], 64, 1), odd[D:])
        gate = jnp.concatenate([turned[3 * D : 4 * D, at], turned[7 * D : 8 * D, at]], axis=0)
        attended = jnp.concatenate([head_0, head_1], axis=0)
        pieces.append(jax.nn.sigmoid(gate) * attended)
    gated = jnp.concatenate(pieces, axis=1)
    gated = jnp.concatenate([gated, jnp.zeros_like(gated)], axis=0).T
    gated = gated.reshape(COLS // 2, 2, HEADS, 8, 128)
    for k in range(HEADS):
        even = gated[:, 0, k].reshape(OWN_POS // 2, 128)
        odd = gated[:, 1, k].reshape(OWN_POS // 2, 128)
        out[k, 0 : OWN_POS // 2, :] = (even + pltpu.roll(odd, 64, 1)).astype(BF16)
        out[k, OWN_POS // 2 : OWN_POS // 2 + 2 * D, :] = merging[:, 0:128]
        out[k, OWN_POS // 2 + 2 * D :, :] = merging[:, 128:256]


Z2_ROWS = 64


def finish_kernel(heads, residual, marks, gain, mapping, out):
    half = OWN_POS // 2
    gated = jnp.concatenate([heads[k, 0:half, :] for k in range(HEADS)], axis=1)
    empty = jnp.zeros((2 * D, WIDTH), BF16)
    blocks = [
        jnp.concatenate([heads[k, half : half + 2 * D, :], heads[k, half + 2 * D :, :]], axis=1)
        for k in range(HEADS)
    ]
    even_rows, odd_rows = [], []
    for block in blocks:
        even_rows += [block, empty]
        odd_rows += [empty, block]
    even = dot(gated, jnp.concatenate(even_rows, axis=0)).reshape(COLS // 2, 1, 8, WIDTH)
    odd = dot(gated, jnp.concatenate(odd_rows, axis=0)).reshape(COLS // 2, 1, 8, WIDTH)
    update = jnp.concatenate([even, odd], axis=1).reshape(OWN_POS, WIDTH)
    refreshed = (residual[...].astype(F32) + update).astype(BF16).astype(F32)
    standard = normed(refreshed, gain[...], WIDTH).astype(BF16)
    factors = (dot(standard, mapping[...]) * marks[:, 0:64]).astype(BF16)

    lane = iota((2 * D, 128), 1)
    source = iota((2 * D, 128), 0)
    position = iota((OWN_POS, 128), 0)
    place = iota((OWN_POS, 128), 1)
    left = dot(factors, one_hot(source == lane % D))
    left = jnp.where(position % 4 == place // D, left, 0.0).astype(BF16)
    left = dot(one_hot(iota((32, OWN_POS), 1) // 4 == iota((32, OWN_POS), 0)), left).astype(BF16)
    right = jnp.zeros((COLS * 16, 128), F32)
    chosen = iota((COLS * 16, OWN_POS), 0)
    block_of = iota((COLS * 16, OWN_POS), 1) // 8
    for k in range(2):
        part = dot(factors, one_hot(source == D + 16 * k + lane // 8))
        part = jnp.where(position % 8 == place % 8, part, 0.0).astype(BF16)
        right = right + dot(one_hot((chosen // 16 == block_of) & (chosen % 16 == k)), part)
    rows = jnp.concatenate(
        [
            refreshed[:, 0:128].reshape(COLS, 8, 128),
            refreshed[:, 128:256].reshape(COLS, 8, 128),
        ],
        axis=1,
    ).astype(BF16)
    for dest in range(COLS):
        out[dest, 0:32, :] = left
    out[:, 32:48, :] = rows
    out[:, 48:64, :] = right.reshape(COLS, 16, 128).astype(BF16)


S2_ROWS = 96


def turn_kernel(second, out, refreshed):
    left = second[:, 0:32, :].reshape(32 * ROWS, 128)
    to, source = iota((512, 512), 0), iota((512, 512), 1)
    left = dot(one_hot((source // 32 == to % 16) & (source % 32 == to // 16)), left).astype(BF16)
    right = second[:, 48:64, :].reshape(16 * ROWS, 128)
    to, source = iota((32, 256), 0), iota((32, 256), 1)
    right = dot(one_hot((source // 16 == to % 16) & (source % 16 == to // 16)), right).astype(BF16)
    for dest in range(SEQS):
        out[dest, 0:64, :] = left[64 * dest : 64 * (dest + 1)]
        out[dest, 64:96, :] = right
    refreshed[...] = second[:, 32:48, :].reshape(ROWS * 16, 128)


H2_ROWS = SEQS * S2_ROWS + ROWS * 16


def copies_kernel(third, refreshed, out):
    for dest in range(HEADS):
        out[dest, 0 : SEQS * S2_ROWS, :] = third[...].reshape(SEQS * S2_ROWS, 128)
        out[dest, SEQS * S2_ROWS :, :] = refreshed[...]


def outer_kernel(last, couple, factor, matrix, sequence_out, pair_out, outer, mixed):
    at = SEQS * S2_ROWS
    low, high = [], []
    for h in range(HEADS):
        rows = last[h, at:, :].astype(F32).reshape(ROWS, 16, 128)
        low.append(rows[:, 0:8])
        high.append(rows[:, 8:16])
    sequence_out[:, :, 0:128] = jnp.concatenate(low, axis=1).astype(BF16)
    sequence_out[:, :, 128:256] = jnp.concatenate(high, axis=1).astype(BF16)

    def gathered(h, row):
        return jnp.concatenate(
            [last[h, S2_ROWS * a + row : S2_ROWS * a + row + ROWS, :] for a in range(SEQS)], axis=0
        )

    mixed[...] = jnp.zeros_like(mixed)
    for q in range(D):
        block = matrix[q]
        for k in range(4):
            mixed[128 * q + D * k : 128 * q + D * (k + 1), 128 * k : 128 * (k + 1)] = block

    left = jnp.concatenate(
        [gathered(h, ROWS * g) for h in range(HEADS) for g in range(4)], axis=1
    )
    for k in range(2):
        found = [dot_first(gathered(h, 64 + ROWS * k), left) for h in range(HEADS)]
        for q in range(16):
            block = jnp.concatenate([f[8 * q : 8 * (q + 1)] for f in found], axis=0).astype(BF16)
            channel = 16 * k + q
            for n in range(16):
                outer[TILE_J * n : TILE_J * (n + 1), 128 * channel : 128 * (channel + 1)] = block[
                    :, 128 * n : 128 * (n + 1)
                ]
    total = dot(outer[...], mixed[...])
    for n in range(16):
        for k in range(4):
            i = 32 * (n % 4 // 2) + 8 * (n // 4) + 4 * (n % 2) + k
            update = total[TILE_J * n : TILE_J * (n + 1), 128 * k : 128 * (k + 1)]
            update = update * factor[:, i : i + 1]
            pair_out[i] = (couple[i].astype(F32) + update).astype(BF16)


def local(
    sequence_matrix,
    sequence_presence,
    couple_matrix,
    couple_delta_selector,
    softmax_scaling_vector,
    couple_scaling_vector,
    couple_logit_matrix,
    query_value_matrices,
    merging_matrix,
    tensor_average_scaling,
    factor_mapping_matrix,
    tensor_average_matrix,
):
    assert sequence_matrix.shape == (ROWS, POS, WIDTH)
    assert couple_matrix.shape == (TILE_I, TILE_J, PAIR)
    seq, col, head = lax.axis_index(SEQ), lax.axis_index("col"), lax.axis_index("head")
    place = jnp.stack([seq, col, head]).astype(jnp.int32)
    first = vmem_call(
        first_kernel,
        shape_of((COLS, Z1_ROWS, 128)),
        sequence_matrix,
        sequence_presence,
        couple_matrix,
        couple_scaling_vector.reshape(1, PAIR),
        couple_logit_matrix,
        scalars=(place[1:2],),
        name="first",
    )
    first = lax.all_to_all(first, "col", 0, 0, tiled=True)
    strips = vmem_call(spread_kernel, shape_of((SEQS, S1_ROWS, 128)), first, name="spread")
    strips = lax.all_to_all(strips, SEQ, 0, 0, tiled=True)
    heads, residual, marks, factor = vmem_call(
        attend_kernel,
        (
            shape_of((HEADS, H1_ROWS, 128)),
            shape_of((OWN_POS, WIDTH)),
            shape_of((OWN_POS, 128), F32),
            shape_of((TILE_J, TILE_I), F32),
        ),
        first,
        strips,
        query_value_matrices.transpose(1, 0, 2),
        softmax_scaling_vector.reshape(1, WIDTH),
        merging_matrix,
        couple_delta_selector,
        scalars=(place,),
        name="attend",
    )
    heads = lax.all_to_all(heads, "head", 0, 0, tiled=True)
    second = vmem_call(
        finish_kernel,
        shape_of((COLS, Z2_ROWS, 128)),
        heads,
        residual,
        marks,
        tensor_average_scaling.reshape(1, WIDTH),
        factor_mapping_matrix,
        name="finish",
    )
    second = lax.all_to_all(second, "col", 0, 0, tiled=True)
    third, refreshed = vmem_call(
        turn_kernel,
        (shape_of((SEQS, S2_ROWS, 128)), shape_of((ROWS * 16, 128))),
        second,
        name="turn",
    )
    third = lax.all_to_all(third, SEQ, 0, 0, tiled=True)
    last = vmem_call(copies_kernel, shape_of((HEADS, H2_ROWS, 128)), third, refreshed, name="copies")
    last = lax.all_to_all(last, "head", 0, 0, tiled=True)
    return tuple(
        vmem_call(
            outer_kernel,
            (shape_of((ROWS, POS, WIDTH)), shape_of((TILE_I, TILE_J, PAIR))),
            last,
            couple_matrix,
            factor,
            tensor_average_matrix.reshape(D, D, PAIR).swapaxes(0, 1),
            scratch=(
                pltpu.VMEM((16 * TILE_J, D * 128), BF16),
                pltpu.VMEM((D * 128, 4 * PAIR), BF16),
            ),
            name="outer",
        )
    )


def solution(mesh):
    torus = Mesh(
        mesh.devices.reshape(2, 4, mesh.shape["col"], mesh.shape["head"]),
        ("seq_0", "seq_1", "col", "head"),
    )
    placed = (
        P(SEQ, "col", None),
        P(SEQ, "col"),
        P(SEQ, "col", None),
        P(SEQ, "col"),
        P(),
        P(),
        P(None, "head"),
        P(None, "head", None),
        P("head", None),
        P(),
        P(),
        P(),
    )
    return jax.shard_map(
        local,
        mesh=torus,
        in_specs=placed,
        out_specs=(P(SEQ, "col", None), P(SEQ, "col", None)),
        check_vma=False,
    )
```

```python
import jax
import jax.numpy as jnp
from jax import lax
from jax.experimental import pallas as pl
from jax.experimental.pallas import tpu as pltpu
from jax.sharding import Mesh
from jax.sharding import PartitionSpec as P

SEQ = ("seq_0", "seq_1")
EPSILON = 1e-05
MASKED_FILL = -1000000000.0
F32 = jnp.float32
BF16 = jnp.bfloat16

SEQS, COLS, HEADS = 8, 16, 4
ROWS, POS, WIDTH = 16, 32, 256
TILE_I, TILE_J, PAIR = 64, 32, 128
ALL_POS = COLS * POS
OWN_POS = ALL_POS // HEADS
D = 32


def iota(shape, dim):
    return lax.broadcasted_iota(jnp.int32, shape, dim)


def dot(a, b):
    return jnp.dot(a, b, preferred_element_type=F32)


def dot_first(a, b):
    return lax.dot_general(a, b, (((0,), (0,)), ((), ())), preferred_element_type=F32)


def dot_last(a, b):
    return lax.dot_general(a, b, (((1,), (1,)), ((), ())), preferred_element_type=F32)


def one_hot(mask):
    return mask.astype(F32).astype(BF16)


def normed(values, gain, width):
    average = jnp.sum(values, axis=-1, keepdims=True) * (1.0 / width)
    centered = values - average
    variance = jnp.sum(centered * centered, axis=-1, keepdims=True) * (1.0 / width)
    return centered * lax.rsqrt(variance + EPSILON) * gain


def vmem_call(
    kernel, out_shapes, *args, hbm=(), scratch=(), flops=1000000, name=None, vmem=48
):
    specs = [pl.BlockSpec(memory_space=pltpu.HBM)] * len(hbm)
    specs += [pl.BlockSpec(memory_space=pltpu.VMEM)] * len(args)
    single = not isinstance(out_shapes, (list, tuple))
    shapes = [out_shapes] if single else list(out_shapes)
    found = pl.pallas_call(
        kernel,
        out_shape=shapes,
        in_specs=specs,
        out_specs=[pl.BlockSpec(memory_space=pltpu.VMEM)] * len(shapes),
        scratch_shapes=list(scratch),
        cost_estimate=pl.CostEstimate(flops=flops, bytes_accessed=1000000, transcendentals=0),
        compiler_params=pltpu.CompilerParams(vmem_limit_bytes=vmem * 1024 * 1024 - 65536),
        name=name,
    )(*hbm, *args)
    return found[0] if single else found


def to_partner(value, distance):
    return lax.ppermute(value, "head", [(k, k ^ distance) for k in range(HEADS)])


def shape_of(dims, dtype=BF16):
    return jax.ShapeDtypeStruct(dims, dtype)


HALF = POS // 2
Z1_MARKS = 2 * HALF + TILE_J
Z1_ROWS = Z1_MARKS + 8


def first_kernel(msa_hbm, presence_hbm, couple_hbm, gain_hbm, logits_hbm, out, msa, presence, couple, gain, logits, sems):
    pairs = (
        (logits_hbm, logits),
        (presence_hbm, presence),
        (gain_hbm, gain),
        (couple_hbm, couple),
        (msa_hbm, msa),
    )
    copies = [pltpu.make_async_copy(x, y, sems.at[k]) for k, (x, y) in enumerate(pairs)]
    for copy in copies:
        copy.start()
    low_row = iota((PAIR, PAIR), 0) < TILE_I
    copies[0].wait()
    rows = logits[...].astype(F32)
    spread = jnp.where(low_row, rows[0:1, :], rows[1:2, :]).astype(BF16)
    place_of_lane = iota((TILE_J, PAIR), 1) % TILE_I
    step = 16

    copies[1].wait()
    marks = presence[...].astype(F32)
    marks = jnp.concatenate([marks] * 4, axis=1)
    marks = jnp.where(iota((ROWS, PAIR), 1) // POS == iota((ROWS, PAIR), 0) % 4, marks, 0.0)
    marks = dot(one_hot(iota((8, ROWS), 1) // 4 == iota((8, ROWS), 0)), marks.astype(BF16))
    marks = marks.astype(BF16)
    copies[2].wait()
    copies[3].wait()
    pair_gain = gain[...]

    def body(k, total):
        block = couple[pl.ds(k * step, step)].astype(F32).reshape(step * TILE_J, PAIR)
        value = normed(block, pair_gain, PAIR).astype(BF16)
        found = dot_last(value, spread)
        for r in range(step):
            row = found[r * TILE_J : (r + 1) * TILE_J]
            total = total + jnp.where(place_of_lane == k * step + r, row, 0.0)
        return total

    bias = jnp.zeros((TILE_J, PAIR), F32)
    for k in range(TILE_I // step):
        bias = body(k, bias)
    bias = bias.astype(BF16)
    copies[4].wait()
    core = lax.axis_index("head") % 2
    for k in range(2):

        @pl.when(core == k)
        def _():
            out[:, 0:HALF, :] = msa[:, HALF * k : HALF * (k + 1), 0:128]
            out[:, HALF : 2 * HALF, :] = msa[:, HALF * k : HALF * (k + 1), 128:256]

    for dest in range(COLS):
        out[dest, 2 * HALF : Z1_MARKS, :] = bias
        out[dest, Z1_MARKS:, :] = marks


S1_ROWS = ALL_POS + 24


def spread_kernel(first, out, raw):
    strip = first[:, 2 * HALF : Z1_MARKS, :].reshape(ALL_POS, PAIR)
    columns = first[lax.axis_index("col"), Z1_MARKS:, :]
    for dest in range(SEQS):
        out[dest, 0:ALL_POS, :] = strip
        out[dest, ALL_POS : ALL_POS + 8, :] = first[2 * dest, Z1_MARKS:, :]
        out[dest, ALL_POS + 8 : ALL_POS + 16, :] = first[2 * dest + 1, Z1_MARKS:, :]
        out[dest, ALL_POS + 16 :, :] = columns
    raw[...] = first[:, 0 : 2 * HALF, :].reshape(COLS * 2 * HALF, 128)


def by_index(arrived, head, k):
    bits = [(k ^ d) == head for d in range(1, HEADS)]
    block = arrived[0]
    for d in range(1, HEADS):
        block = jnp.where(bits[d - 1], arrived[d], block)
    return block


def project_kernel(
    first, raw, raw_1, weights, gain, rounded_out, turned_out, key_bias, own_marks, residual
):
    col, head = lax.axis_index("col"), lax.axis_index("head")
    own_half, other_half = raw[...].astype(F32), raw_1[...].astype(F32)
    low, high = [], []
    for k in range(2):
        rows = jnp.where(head % 2 == k, own_half, other_half).reshape(COLS, 1, 2 * HALF, 128)
        low.append(rows[:, :, 0:HALF])
        high.append(rows[:, :, HALF:])
    low = jnp.concatenate(low, axis=1).reshape(ALL_POS, 128)
    high = jnp.concatenate(high, axis=1).reshape(ALL_POS, 128)
    rows = jnp.concatenate([low, high], axis=1)
    by_owner = rows.reshape(COLS, HEADS, 8, WIDTH)
    own = jnp.zeros((COLS, 8, WIDTH), F32)
    for k in range(HEADS):
        own = own + jnp.where(head == k, by_owner[:, k], 0.0)
    residual[...] = own.reshape(OWN_POS, WIDTH).astype(BF16)
    standard = normed(rows, gain[...], WIDTH).astype(BF16)
    both = jnp.concatenate([weights[0], weights[1]], axis=1)
    rounded = dot(standard, both).astype(BF16)
    rounded_out[...] = rounded
    turned_out[...] = rounded.astype(F32).T.astype(BF16)

    packed = first[:, Z1_MARKS:, :].reshape(COLS * 8, 128)
    shape = (COLS, COLS * 8)
    picked = dot(one_hot(iota(shape, 1) == iota(shape, 0) * 8 + col // 4), packed).astype(BF16)
    shape = (128, POS)
    picked = dot(picked, one_hot(iota(shape, 0) == POS * (col % 4) + iota(shape, 1))).astype(BF16)
    shape = (ALL_POS, COLS)
    picked = dot(one_hot(iota(shape, 0) // POS == iota(shape, 1)), picked)
    shape = (ALL_POS, POS)
    picked = jnp.where(iota(shape, 0) % POS == iota(shape, 1), picked, 0.0).astype(BF16)
    marks = dot(picked, jnp.ones((POS, 128), BF16))
    key_bias[...] = ((1.0 - marks) * MASKED_FILL).astype(BF16)
    by_owner = marks.reshape(COLS, HEADS, 8, 128)
    own = jnp.zeros((COLS, 8, 128), F32)
    for k in range(HEADS):
        own = own + jnp.where(head == k, by_owner[:, k], 0.0)
    own_marks[...] = own.reshape(OWN_POS, 128)


def count_kernel(strips, keep, factor):
    def presence(k):
        at = ALL_POS + 8 * k
        return strips[:, at : at + 8, :].reshape(SEQS * 8, 128)

    first_rows, second_rows, columns = presence(0), presence(1), presence(2)
    count = jnp.zeros((TILE_J, TILE_I), F32)
    for k in range(4):
        shape = (128, TILE_I)
        lane, place = iota(shape, 0) - POS * k, iota(shape, 1)
        rows = dot(first_rows, one_hot((lane == place) & (place < POS)))
        rows = rows + dot(second_rows, one_hot((lane == place - POS) & (place >= POS)))
        shape = (128, TILE_J)
        found = dot(columns, one_hot(iota(shape, 0) - POS * k == iota(shape, 1)))
        count = count + dot_first(found.astype(BF16), rows.astype(BF16))
    same = one_hot(iota((TILE_I, TILE_I), 0) == iota((TILE_I, TILE_I), 1))
    kept = dot_first(keep[...].astype(F32).astype(BF16), same)
    factor[...] = kept / (1.0 + count)


H1_ROWS = OWN_POS // 2 + 2 * 2 * D


def attend_kernel(strips, rounded_in, turned_in, key_bias_in, merging, out):
    rounded = rounded_in[...]
    turned = turned_in[...].astype(F32)
    key_bias = key_bias_in[...].astype(F32)
    score_scale = D ** (-0.5)
    low = iota((D, 128), 1) < TILE_I
    zero = jnp.zeros((D, 128), F32)
    values = jnp.concatenate([turned[2 * D : 3 * D], turned[6 * D : 7 * D]], axis=0).astype(BF16)

    def tile_attended(a, first_queries, second_queries):
        queries = jnp.concatenate(
            [
                zero,
                jnp.where(low, first_queries, 0.0),
                zero,
                zero,
                zero,
                jnp.where(low, 0.0, second_queries),
                zero,
                zero,
            ],
            axis=0,
        ).astype(BF16)
        scores = dot(rounded, queries) * score_scale
        scores = scores + strips[a, 0:ALL_POS, :].astype(F32) + key_bias
        top = jnp.max(scores, axis=0, keepdims=True)
        raised = jnp.exp(scores - top)
        shares = (raised / jnp.sum(raised, axis=0, keepdims=True)).astype(BF16)
        return dot(values, shares)

    pieces = []
    for t in range(4):
        at = slice(128 * t, 128 * (t + 1))
        q0, q1 = turned[0:D, at], turned[4 * D : 5 * D, at]
        even = tile_attended(2 * t, q0, pltpu.roll(q1, 64, 1))
        odd = tile_attended(2 * t + 1, pltpu.roll(q0, 64, 1), q1)
        head_0 = jnp.where(low, even[0:D], pltpu.roll(odd[0:D], 64, 1))
        head_1 = jnp.where(low, pltpu.roll(even[D:], 64, 1), odd[D:])
        gate = jnp.concatenate([turned[3 * D : 4 * D, at], turned[7 * D : 8 * D, at]], axis=0)
        attended = jnp.concatenate([head_0, head_1], axis=0)
        pieces.append(jax.nn.sigmoid(gate) * attended)
    gated = jnp.concatenate(pieces, axis=1)
    gated = jnp.concatenate([gated, jnp.zeros_like(gated)], axis=0).T
    gated = gated.reshape(COLS // 2, 2, HEADS, 8, 128)
    for k in range(HEADS):
        even = gated[:, 0, k].reshape(OWN_POS // 2, 128)
        odd = gated[:, 1, k].reshape(OWN_POS // 2, 128)
        out[k, 0 : OWN_POS // 2, :] = (even + pltpu.roll(odd, 64, 1)).astype(BF16)
        out[k, OWN_POS // 2 : OWN_POS // 2 + 2 * D, :] = merging[:, 0:128]
        out[k, OWN_POS // 2 + 2 * D :, :] = merging[:, 128:256]


Z2_ROWS = 56


def finish_kernel(heads, residual, marks, gain, mapping, out):
    half = OWN_POS // 2
    gated = jnp.concatenate([heads[k, 0:half, :] for k in range(HEADS)], axis=1)
    empty = jnp.zeros((2 * D, WIDTH), BF16)
    blocks = [
        jnp.concatenate([heads[k, half : half + 2 * D, :], heads[k, half + 2 * D :, :]], axis=1)
        for k in range(HEADS)
    ]
    even_rows, odd_rows = [], []
    for block in blocks:
        even_rows += [block, empty]
        odd_rows += [empty, block]
    even = dot(gated, jnp.concatenate(even_rows, axis=0)).reshape(COLS // 2, 1, 8, WIDTH)
    odd = dot(gated, jnp.concatenate(odd_rows, axis=0)).reshape(COLS // 2, 1, 8, WIDTH)
    update = jnp.concatenate([even, odd], axis=1).reshape(OWN_POS, WIDTH)
    refreshed = (residual[...].astype(F32) + update).astype(BF16).astype(F32)
    standard = normed(refreshed, gain[...], WIDTH).astype(BF16)
    factors = (dot_last(standard, mapping[...]) * marks[:, 0:64]).astype(BF16)

    lane = iota((2 * D, 128), 1)
    source = iota((2 * D, 128), 0)
    position = iota((OWN_POS, 128), 0)
    place = iota((OWN_POS, 128), 1)
    left = dot(factors, one_hot(source == lane % D))
    left = jnp.where(position % 4 == place // D, left, 0.0).astype(BF16)
    left = dot(one_hot(iota((32, OWN_POS), 1) // 4 == iota((32, OWN_POS), 0)), left).astype(BF16)
    right = jnp.zeros((COLS * 8, 128), F32)
    chosen = iota((COLS * 8, OWN_POS), 0)
    block_of = iota((COLS * 8, OWN_POS), 1) // 8
    for k in range(2):
        part = dot(factors, one_hot(source == D + 16 * k + lane // 8))
        part = jnp.where(position % 8 == place % 8, part, 0.0).astype(BF16)
        right = right + dot(one_hot((chosen // 8 == block_of) & (chosen % 8 == k)), part)
    rows = jnp.concatenate(
        [
            refreshed[:, 0:128].reshape(COLS, 8, 128),
            refreshed[:, 128:256].reshape(COLS, 8, 128),
        ],
        axis=1,
    ).astype(BF16)
    for dest in range(COLS):
        out[dest, 0:32, :] = left
    out[:, 32:48, :] = rows
    out[:, 48:56, :] = right.reshape(COLS, 8, 128).astype(BF16)


S2_ROWS = 96
LAST_ROWS = SEQS * S2_ROWS + ROWS * 16


def join_kernel(third, refreshed, out):
    out[0 : SEQS * S2_ROWS, :] = third[...].reshape(SEQS * S2_ROWS, 128)
    out[SEQS * S2_ROWS :, :] = refreshed[...]


def turn_kernel(second, out, refreshed):
    left = second[:, 0:32, :].reshape(32 * ROWS, 128)
    to, source = iota((512, 512), 0), iota((512, 512), 1)
    left = dot(one_hot((source // 32 == to % 16) & (source % 32 == to // 16)), left).astype(BF16)
    right = second[:, 48:56, :].reshape(8 * ROWS, 128)
    to, source = iota((32, 128), 0), iota((32, 128), 1)
    right = dot(one_hot((source // 8 == to % 16) & (source % 8 == to // 16)), right).astype(BF16)
    for dest in range(SEQS):
        out[dest, 0:64, :] = left[64 * dest : 64 * (dest + 1)]
        out[dest, 64:96, :] = right
    refreshed[...] = second[:, 32:48, :].reshape(ROWS * 16, 128)


def outer_kernel(*refs):
    last = refs[0:HEADS]
    couple, factor, matrix, sequence_out, pair_out, outer, mixed = refs[HEADS:]
    head = lax.axis_index("head")
    end = SEQS * S2_ROWS
    arrived = [r[end:, :].astype(F32) for r in last]
    low, high = [], []
    for k in range(HEADS):
        rows = by_index(arrived, head, k).reshape(ROWS, 16, 128)
        low.append(rows[:, 0:8])
        high.append(rows[:, 8:16])
    sequence_out[:, :, 0:128] = jnp.concatenate(low, axis=1).astype(BF16)
    sequence_out[:, :, 128:256] = jnp.concatenate(high, axis=1).astype(BF16)

    factors = [r[0:end, :] for r in last]
    factors = [by_index(factors, head, k) for k in range(HEADS)]

    def gathered(h, row):
        return jnp.concatenate(
            [factors[h][S2_ROWS * a + row : S2_ROWS * a + row + ROWS] for a in range(SEQS)], axis=0
        )

    mixed[...] = jnp.zeros_like(mixed)
    for q in range(D):
        block = matrix[q]
        for k in range(4):
            mixed[128 * q + D * k : 128 * q + D * (k + 1), 128 * k : 128 * (k + 1)] = block

    left = jnp.concatenate(
        [gathered(h, ROWS * g) for h in range(HEADS) for g in range(4)], axis=1
    )
    for k in range(2):
        found = [dot_first(gathered(h, 64 + ROWS * k), left) for h in range(HEADS)]
        for q in range(16):
            block = jnp.concatenate([f[8 * q : 8 * (q + 1)] for f in found], axis=0).astype(BF16)
            channel = 16 * k + q
            for n in range(16):
                outer[TILE_J * n : TILE_J * (n + 1), 128 * channel : 128 * (channel + 1)] = block[
                    :, 128 * n : 128 * (n + 1)
                ]
    total = dot(outer[...], mixed[...])
    for n in range(16):
        for k in range(4):
            i = 32 * (n % 4 // 2) + 8 * (n // 4) + 4 * (n % 2) + k
            update = total[TILE_J * n : TILE_J * (n + 1), 128 * k : 128 * (k + 1)]
            update = update * factor[:, i : i + 1]
            pair_out[i] = (couple[i].astype(F32) + update).astype(BF16)


def local(
    sequence_matrix,
    sequence_presence,
    couple_matrix,
    couple_delta_selector,
    softmax_scaling_vector,
    couple_scaling_vector,
    couple_logit_matrix,
    query_value_matrices,
    merging_matrix,
    tensor_average_scaling,
    factor_mapping_matrix,
    tensor_average_matrix,
):
    assert sequence_matrix.shape == (ROWS, POS, WIDTH)
    assert couple_matrix.shape == (TILE_I, TILE_J, PAIR)
    first = vmem_call(
        first_kernel,
        shape_of((COLS, Z1_ROWS, 128)),
        hbm=(
            sequence_matrix,
            sequence_presence,
            couple_matrix,
            couple_scaling_vector.reshape(1, PAIR),
            couple_logit_matrix.T,
        ),
        scratch=(
            pltpu.VMEM((ROWS, POS, WIDTH), BF16),
            pltpu.VMEM((ROWS, POS), jnp.int32),
            pltpu.VMEM((TILE_I, TILE_J, PAIR), BF16),
            pltpu.VMEM((1, PAIR), F32),
            pltpu.VMEM((2, PAIR), BF16),
            pltpu.SemaphoreType.DMA((5,)),
        ),
        vmem=64,
        name="first",
    )
    first = lax.all_to_all(first, "col", 0, 0, tiled=True)
    strips, raw = vmem_call(
        spread_kernel,
        (shape_of((SEQS, S1_ROWS, 128)), shape_of((COLS * 2 * HALF, 128))),
        first,
        name="spread",
    )
    raws = [raw, to_partner(raw, 1)]
    strips = lax.all_to_all(strips, SEQ, 0, 0, tiled=True)
    rounded, turned, key_bias, marks, residual = vmem_call(
        project_kernel,
        (
            shape_of((ALL_POS, WIDTH)),
            shape_of((WIDTH, ALL_POS)),
            shape_of((ALL_POS, 128)),
            shape_of((OWN_POS, 128), F32),
            shape_of((OWN_POS, WIDTH)),
        ),
        first,
        *raws,
        query_value_matrices.transpose(1, 0, 2),
        softmax_scaling_vector.reshape(1, WIDTH),
        flops=400000000,
        name="project",
    )
    heads = vmem_call(
        attend_kernel,
        shape_of((HEADS, H1_ROWS, 128)),
        strips,
        rounded,
        turned,
        key_bias,
        merging_matrix,
        flops=600000000,
        name="attend",
    )
    heads = lax.all_to_all(heads, "head", 0, 0, tiled=True)
    factor = vmem_call(
        count_kernel,
        shape_of((TILE_J, TILE_I), F32),
        strips,
        couple_delta_selector,
        flops=100000000,
        name="count",
    )
    second = vmem_call(
        finish_kernel,
        shape_of((COLS, Z2_ROWS, 128)),
        heads,
        residual,
        marks,
        tensor_average_scaling.reshape(1, WIDTH),
        factor_mapping_matrix.T,
        flops=100000000,
        name="finish",
    )
    second = lax.all_to_all(second, "col", 0, 0, tiled=True)
    third, refreshed = vmem_call(
        turn_kernel,
        (shape_of((SEQS, S2_ROWS, 128)), shape_of((ROWS * 16, 128))),
        second,
        name="turn",
    )
    third = lax.all_to_all(third, SEQ, 0, 0, tiled=True)
    last = vmem_call(join_kernel, shape_of((LAST_ROWS, 128)), third, refreshed, name="join")
    across = to_partner(last, 2)
    last = [last, to_partner(last, 1), across, to_partner(across, 1)]
    return tuple(
        vmem_call(
            outer_kernel,
            (shape_of((ROWS, POS, WIDTH)), shape_of((TILE_I, TILE_J, PAIR))),
            *last,
            couple_matrix,
            factor,
            tensor_average_matrix.reshape(D, D, PAIR).swapaxes(0, 1),
            scratch=(
                pltpu.VMEM((16 * TILE_J, D * 128), BF16),
                pltpu.VMEM((D * 128, 4 * PAIR), BF16),
            ),
            flops=2000000000,
            name="outer",
        )
    )


def solution(mesh):
    torus = Mesh(
        mesh.devices.reshape(2, 4, mesh.shape["col"], mesh.shape["head"]),
        ("seq_0", "seq_1", "col", "head"),
    )
    placed = (
        P(SEQ, "col", None),
        P(SEQ, "col"),
        P(SEQ, "col", None),
        P(SEQ, "col"),
        P(),
        P(),
        P(None, "head"),
        P(None, "head", None),
        P("head", None),
        P(),
        P(),
        P(),
    )
    return jax.shard_map(
        local,
        mesh=torus,
        in_specs=placed,
        out_specs=(P(SEQ, "col", None), P(SEQ, "col", None)),
        check_vma=False,
    )
```
